512 devices in a mesh: wide: 128 (over x, z, core), narrow: 4 (over y).
Axes of the slice: x: 4, y: 4, z: 16, core: 2. Of those that a mesh axis runs over, the one named last changes fastest.
Arguments:
- fields: bfloat16 [256, 524288], P('wide', 'narrow'), may hold values from -8 to 8
- counts: int32 [4, 128], P(None, 'wide'), may hold values from 1 to 8, as said below
- obs_index: int32 [4, 128, 8, 512], P('narrow', 'wide'), may hold values from 0 to 1023
- obs_value: float32 [4, 128, 8, 512], P('narrow', 'wide'), may hold values from -6 to 6
- obs_weight: bfloat16 [4, 128, 8, 512], P('narrow', 'wide'), may hold values from 1 to 16
Outputs:
- analysis: bfloat16 [256, 524288], P('wide', 'narrow')
The draws below stay inside these ranges and needn't reach their ends.
Inputs may be any that keep to these rules, and one draw needn't show every extreme that they name: `counts`: tiles with the same wide index form a group of 4; in each group exactly one tile owns 6 to 8 patches and every other tile owns 1 to 4. `obs_index`: slots numbered at or beyond the tile's count are never read.
All inputs are finite; a program needn't handle non-finite values.
Results may differ from the reference program's by a relative error of at most 0.009.
Values may be sent and summed in bfloat16 or wider, within the bound.
A program may use at most 64 MiB of HBM per device.

```python
import math
import jax
import jax.numpy as jnp
from jax import lax

K = 256
NOBS = 512
PMAX = 8
LOCAL = 5
NS_ITERS = 6
CELL_DEV = 1024
NCELL = 524288
N_WIDE = 128
N_NARROW = 4


def draw_fields(key, part):
    key_base, key_scale, key_noise = jax.random.split(jax.random.fold_in(key, 11), 3)
    base_field = jax.random.normal(key_base, (1, NCELL), jnp.float32)
    spread = jnp.exp(jax.random.uniform(key_scale, (1, NCELL), jnp.float32, math.log(0.3), math.log(1.5)))
    noise = jax.random.normal(key_noise, (K, NCELL), jnp.float32)
    return jnp.clip(base_field + spread * noise, -8.0, 8.0).astype(jnp.bfloat16)


def draw_counts(key, part):
    key_heavy, key_pick, key_light = jax.random.split(jax.random.fold_in(key, 23), 3)
    heavy_row = jax.random.randint(key_pick, (1, N_WIDE), 0, N_NARROW)
    heavy_count = jax.random.randint(key_heavy, (1, N_WIDE), LOCAL + 1, PMAX + 1)
    light_count = jax.random.randint(key_light, (N_NARROW, N_WIDE), 1, LOCAL)
    row_ids = lax.broadcasted_iota(jnp.int32, (N_NARROW, N_WIDE), 0)
    return jnp.where(row_ids == heavy_row, heavy_count, light_count).astype(jnp.int32)


def set_ends(values, stream_key, low, high):
    longest = values.shape.index(max(values.shape))
    spots = []
    for shift in (0, 1):
        where = [jax.random.randint(jax.random.fold_in(stream_key, axis), (), 0, length) for axis, length in enumerate(values.shape)]
        where[longest] = (where[longest] + shift) % values.shape[longest]
        spots.append(tuple(where))
    return values.at[spots[0]].set(low).at[spots[1]].set(high)


def levels(own_key, shape, shards, low, top_value):
    level, own = 1.0, jax.random.fold_in(own_key, 6)
    for axis_at, shards_of in shards:
        steps = jnp.exp(jax.random.uniform(jax.random.fold_in(own, axis_at), (shards_of,), jnp.float32, low / len(shards), top_value / len(shards)))
        level = level * jnp.repeat(steps, shape[axis_at] // shards_of).reshape([-1 if axis == axis_at else 1 for axis in range(len(shape))])
    return level


def gaussian(own_key, dims, width, reach, cuts=(), kind=jnp.bfloat16):
    array = jax.random.normal(own_key, dims, jnp.float32) * width
    if len(cuts) > 0:
        array = levels(own_key, dims, cuts, -0.22, 0.18) * array
    return jnp.clip(array, min=-reach, max=reach).astype(kind)


def setup_inputs(seed: int = 0) -> dict:
    key_list = jax.random.split(jax.random.key(seed), 6)
    fields = draw_fields(jax.random.fold_in(key_list[5], 71), 0)
    counts = draw_counts(jax.random.fold_in(key_list[5], 71), 0)
    obs_index = set_ends(jax.random.randint(key_list[2], (N_NARROW, N_WIDE, PMAX, NOBS), 0, CELL_DEV), jax.random.fold_in(key_list[2], 1), 0, CELL_DEV - 1).astype(jnp.int32)
    obs_value = gaussian(key_list[3], (N_NARROW, N_WIDE, PMAX, NOBS), 1.5, 6.0, ((0, 4), (1, 128)), jnp.float32)
    obs_weight = jnp.clip(jnp.exp(math.log(16.0) - 2.7725887 * jax.random.uniform(key_list[4], (N_NARROW, N_WIDE, PMAX, NOBS), jnp.float32) ** levels(key_list[4], (N_NARROW, N_WIDE, PMAX, NOBS), ((0, 4), (1, 128)), -0.2, 0.2)), 1.0, 16.0).astype(jnp.bfloat16)
    return dict(fields=fields, counts=counts, obs_index=obs_index, obs_value=obs_value, obs_weight=obs_weight)


def prepare_slots(observed, weighted, innovation):
    members = observed.shape[0]
    highest = lax.Precision.HIGHEST
    obs_float = observed.astype(jnp.float32)
    identity_matrix = jnp.eye(members, dtype=jnp.float32)
    gram_matrix = jnp.einsum('ksn,lsn->skl', weighted.astype(jnp.float32), obs_float, precision=highest)
    gram_matrix = gram_matrix + (members - 1.0) * identity_matrix
    scale_value = jnp.sqrt(lax.optimization_barrier(jnp.sum(gram_matrix * gram_matrix, axis=(1, 2))))
    right_side = jnp.einsum('ksn,sn->sk', obs_float, innovation.astype(jnp.float32), precision=highest)
    iterate = (gram_matrix / scale_value[:, None, None]).astype(jnp.bfloat16)
    return (iterate, scale_value, right_side)

def newton_steps(iterate):
    members = iterate.shape[1]
    highest = lax.Precision.HIGHEST
    identity_matrix = jnp.eye(members, dtype=jnp.float32)
    root_matrix = jnp.broadcast_to(identity_matrix, iterate.shape).astype(jnp.bfloat16)
    for iteration in range(NS_ITERS):
        product = jnp.einsum('skl,slm->skm', root_matrix.astype(jnp.float32), iterate.astype(jnp.float32), precision=highest)
        factor = (1.5 * identity_matrix - 0.5 * product).astype(jnp.bfloat16)
        factor_float = factor.astype(jnp.float32)
        next_iterate = jnp.einsum('skl,slm->skm', iterate.astype(jnp.float32), factor_float, precision=highest).astype(jnp.bfloat16)
        root_matrix = jnp.einsum('skl,slm->skm', factor_float, root_matrix.astype(jnp.float32), precision=highest).astype(jnp.bfloat16)
        iterate = next_iterate
    return root_matrix

def finish_slots(root_matrix, scale_value, right_side):
    members = root_matrix.shape[1]
    highest = lax.Precision.HIGHEST
    root_float = root_matrix.astype(jnp.float32)
    inner_vector = jnp.einsum('skl,sl->sk', root_float, right_side, precision=highest)
    mean_shift = jnp.einsum('skl,sl->sk', root_float, inner_vector, precision=highest) / scale_value[:, None]
    patch_weight = jnp.sqrt((members - 1.0) / scale_value)[:, None, None] * root_float + mean_shift[:, :, None]
    return patch_weight.astype(jnp.bfloat16)

def solve_slots(observed, weighted, innovation):
    iterate, scale_value, right_side = prepare_slots(observed, weighted, innovation)
    return finish_slots(newton_steps(iterate), scale_value, right_side)

def combine_blocks(anomaly, member_mean, patch_weights, patch_count):
    members, cell_total = anomaly.shape
    slot_total = patch_weights.shape[0]
    block_ids = jnp.arange(slot_total, dtype=jnp.int32)
    owner_patch = block_ids * patch_count // slot_total
    pick_table = (owner_patch[:, None] == block_ids[None, :]).astype(jnp.float32)
    chosen = jnp.einsum('bp,pkl->bkl', pick_table, patch_weights.astype(jnp.float32), precision=lax.Precision.HIGHEST)
    blocks = anomaly.astype(jnp.float32).reshape(members, slot_total, cell_total // slot_total)
    result = jnp.einsum('bkl,kbc->lbc', chosen, blocks, precision=lax.Precision.HIGHEST)
    result = result + member_mean.reshape(1, slot_total, cell_total // slot_total)
    return result.reshape(members, cell_total).astype(jnp.bfloat16)

def analyse_tile(tile_fields, patch_count, indices, obs_values, weight_tile):
    members = tile_fields.shape[0]
    member_mean = lax.optimization_barrier(jnp.sum(tile_fields.astype(jnp.float32), axis=0)) / members
    anomaly = (tile_fields.astype(jnp.float32) - member_mean[None, :]).astype(jnp.bfloat16)
    observed = jnp.take(anomaly, indices, axis=1)
    obs_mean = jnp.take(member_mean, indices, axis=0)
    weight_float = weight_tile.astype(jnp.float32)
    weighted = (observed.astype(jnp.float32) * weight_float[None]).astype(jnp.bfloat16)
    innovation = (weight_float * (obs_values - obs_mean)).astype(jnp.bfloat16)
    patch_weights = solve_slots(observed, weighted, innovation)
    return combine_blocks(anomaly, member_mean, patch_weights, patch_count)

def reference(fields, counts, obs_index, obs_value, obs_weight):
    tile_total = N_NARROW * N_WIDE
    counts_flat = counts.reshape(tile_total)
    index_flat = obs_index.reshape(tile_total, PMAX, NOBS)
    value_flat = obs_value.reshape(tile_total, PMAX, NOBS)
    weight_flat = obs_weight.reshape(tile_total, PMAX, NOBS)

    def one_tile(tile_number, output):
        tile_number = tile_number.astype(jnp.int32)
        start = (tile_number * CELL_DEV).astype(jnp.int32)
        tile_fields = lax.dynamic_slice_in_dim(fields, start, CELL_DEV, 1)
        result = analyse_tile(tile_fields, counts_flat[tile_number], index_flat[tile_number], value_flat[tile_number], weight_flat[tile_number])
        return lax.dynamic_update_slice_in_dim(output, result.astype(output.dtype), start, 1)
    output = jnp.zeros((K, NCELL), jnp.bfloat16)
    return lax.fori_loop(0, tile_total, one_tile, output)
```

```python
import functools

import jax
import jax.numpy as jnp
from jax import lax
from jax.experimental import pallas as pl
from jax.experimental.pallas import tpu as pltpu
from jax.sharding import PartitionSpec as P

MEMBERS = 256
NOBS = 512
SLOTS = 8
CELLS = 1024
BLOCK = 128
NS_ITERS = 6
WIDE = 128
CHIPS_X, CHIPS_Z, CORES = 4, 16, 2
PHASES = 4
LANES = 4
MESH = pl.DeviceIdType.MESH
F32, BF16 = jnp.float32, jnp.bfloat16


def dot(a, b):
    return lax.dot_general(a, b, (((1,), (0,)), ((), ())), preferred_element_type=F32)


def dot_t(a, b):
    return lax.dot_general(a, b, (((1,), (1,)), ((), ())), preferred_element_type=F32)


def three_rows(row):
    high = row.astype(BF16).astype(F32)
    rest = row - high
    middle = rest.astype(BF16).astype(F32)
    low = rest - middle
    at = lax.broadcasted_iota(jnp.int32, (16, row.shape[1]), 0)
    rows = jnp.where(at == 0, high, jnp.where(at == 1, middle, jnp.where(at == 2, low, 0.0)))
    return rows.astype(BF16)


def diagonal(value):
    rows = lax.broadcasted_iota(jnp.int32, (MEMBERS, MEMBERS), 0)
    columns = lax.broadcasted_iota(jnp.int32, (MEMBERS, MEMBERS), 1)
    return jnp.where(rows == columns, value, 0.0)


def build_picks(index_ref, pick_ref):
    def one(step, carry):
        slot, part = step // 4, lax.rem(step, 4)
        cells = lax.broadcasted_iota(jnp.int32, (CELLS // 4, NOBS), 0) + part * (CELLS // 4)
        wanted = index_ref[0, 0, pl.ds(slot, 1), :]
        hit = jnp.where(cells == wanted, 1.0, 0.0).astype(BF16)
        pick_ref[slot, pl.ds(pl.multiple_of(part * (CELLS // 4), CELLS // 4), CELLS // 4), :] = hit
        return carry

    lax.fori_loop(0, SLOTS * 4, one, 0)


def load_tile(in_ref, anomaly_ref, mean_ref):
    for block in range(SLOTS):
        columns = slice(block * BLOCK, (block + 1) * BLOCK)
        part = in_ref[:, block].reshape(MEMBERS, BLOCK).astype(F32)
        mean = jnp.sum(part, axis=0, keepdims=True) / MEMBERS
        mean_ref[:, columns] = mean
        anomaly_ref[:MEMBERS, columns] = (part - mean).astype(BF16)
        anomaly_ref[MEMBERS:, columns] = three_rows(mean)


def solve(value_ref, weight_ref, pick_ref, anomaly_ref, seen_ref, heavy_ref, iterate_ref, root_ref, factor_ref, side_ref, scale_ref, patch_ref):
    half = diagonal(1.5)

    def group(step, carry):
        first = step * LANES
        for lane in range(LANES):
            slot = first + lane
            taken = dot(anomaly_ref[...], pick_ref[slot])
            seen_ref[lane] = taken[:MEMBERS].astype(BF16)
            seen_mean = jnp.sum(taken[MEMBERS:], axis=0, keepdims=True)
            weight = weight_ref[pl.ds(slot, 1), :]
            heavy_ref[lane] = (seen_ref[lane].astype(F32) * weight).astype(BF16)
            innovation = (weight * (value_ref[0, 0, pl.ds(slot, 1), :] - seen_mean)).astype(BF16)
            side_ref[lane] = dot_t(jnp.broadcast_to(innovation, (16, NOBS)), seen_ref[lane])[:8]
        for lane in range(LANES):
            gram = dot_t(seen_ref[lane], heavy_ref[lane]) + diagonal(MEMBERS - 1.0)
            scale = jnp.sqrt(jnp.sum(jnp.sum(gram * gram, axis=0, keepdims=True), axis=1, keepdims=True))
            scale_ref[lane] = jnp.broadcast_to(scale, (8, 128))
            iterate_ref[lane] = (gram * (1.0 / scale)).astype(BF16)
        for lane in range(LANES):
            root_ref[lane] = (half - 0.5 * iterate_ref[lane].astype(F32)).astype(BF16)
        for lane in range(LANES):
            iterate_ref[lane] = dot(root_ref[lane], iterate_ref[lane]).astype(BF16)

        def newton(iteration, carry):
            for lane in range(LANES):
                factor_ref[lane] = (half - 0.5 * dot(iterate_ref[lane], root_ref[lane])).astype(BF16)
            for lane in range(LANES):
                iterate_ref[lane] = dot(factor_ref[lane], iterate_ref[lane]).astype(BF16)
                root_ref[lane] = dot(root_ref[lane], factor_ref[lane]).astype(BF16)
            return carry

        lax.fori_loop(1, NS_ITERS - 1, newton, 0)
        for lane in range(LANES):
            factor_ref[lane] = (half - 0.5 * dot(iterate_ref[lane], root_ref[lane])).astype(BF16)
        for lane in range(LANES):
            root_ref[lane] = dot(root_ref[lane], factor_ref[lane]).astype(BF16)
        for lane in range(LANES):
            inner = jnp.sum(dot(three_rows(side_ref[lane][:1]), root_ref[lane]), axis=0, keepdims=True)
            side_ref[lane] = jnp.broadcast_to(inner, (8, MEMBERS))
        for lane in range(LANES):
            scale = scale_ref[lane][:1, :1]
            shift = jnp.sum(dot(three_rows(side_ref[lane][:1]), root_ref[lane]), axis=0, keepdims=True) / scale
            patch = jnp.sqrt((MEMBERS - 1.0) / scale) * root_ref[lane].astype(F32) + shift
            patch_ref[first + lane] = patch.astype(BF16)
        return carry

    lax.fori_loop(0, SLOTS // LANES, group, 0)


def combine(count, patch_ref, anomaly_ref, mean_ref, out_ref):
    for block in range(SLOTS):
        columns = slice(block * BLOCK, (block + 1) * BLOCK)
        slot = (block * count) // SLOTS
        result = dot(patch_ref[slot], anomaly_ref[:MEMBERS, columns]) + mean_ref[:, columns]
        out_ref[:, block] = result.astype(BF16).reshape(MEMBERS // 2, 2, BLOCK)


def kernel(
    fields_ref, counts_ref, index_ref, value_ref, weight_ref, out_ref,
    in_ref, back_ref, pick_ref, anomaly_ref, mean_ref, seen_ref, heavy_ref,
    iterate_ref, root_ref, factor_ref, side_ref, scale_ref, patch_ref,
    wide_weight_ref, send_sem, in_sem, reply_sem, out_sem,
):
    me = lax.axis_index("wide")
    x, z, core = me // (CHIPS_Z * CORES), lax.rem(me // CORES, CHIPS_Z), lax.rem(me, CORES)
    in_ref[me] = fields_ref[me]
    barrier = pltpu.get_barrier_semaphore()

    def greet(step, carry):
        peer = lax.rem(me + step, WIDE)
        pl.semaphore_signal(barrier, inc=1, device_id={"wide": peer}, device_id_type=MESH)
        return carry

    lax.fori_loop(1, WIDE, greet, 0)
    wide_weight_ref[...] = weight_ref[0, 0].astype(F32)
    build_picks(index_ref, pick_ref)
    pl.semaphore_wait(barrier, WIDE - 1)

    def send(step, carry):
        phase = step // (WIDE // PHASES)
        rest = lax.rem(step, WIDE // PHASES)
        hop, rest = rest // (CHIPS_X * CORES), lax.rem(rest, CHIPS_X * CORES)
        to_z = PHASES * lax.rem(z // PHASES + hop, CHIPS_Z // PHASES) + phase
        to_x = lax.rem(x + rest // CORES, CHIPS_X)
        to_core = lax.rem(core + rest, CORES)
        peer = (to_x * CHIPS_Z + to_z) * CORES + to_core

        @pl.when(peer != me)
        def _():
            pltpu.make_async_remote_copy(
                fields_ref.at[peer], in_ref.at[me], send_sem, in_sem,
                device_id={"wide": peer}, device_id_type=MESH,
            ).start()

        return carry

    lax.fori_loop(0, WIDE, send, 0)
    others = in_ref.at[pl.ds(0, WIDE - 1)]
    pltpu.make_async_copy(others, others, in_sem).wait()
    load_tile(in_ref, anomaly_ref, mean_ref)
    solve(value_ref, wide_weight_ref, pick_ref, anomaly_ref, seen_ref, heavy_ref, iterate_ref, root_ref, factor_ref, side_ref, scale_ref, patch_ref)
    combine(counts_ref[lax.axis_index("narrow"), 0], patch_ref, anomaly_ref, mean_ref, back_ref)
    out_ref[me] = back_ref[me]

    def reply(step, carry):
        hop, rest = step // (CHIPS_X * CORES), lax.rem(step, CHIPS_X * CORES)
        side = (hop + 1) // 2
        to_z = lax.rem(z + CHIPS_Z // 2 + side * (1 - 2 * lax.rem(hop, 2)) + CHIPS_Z, CHIPS_Z)
        to_x = lax.rem(x + rest // CORES, CHIPS_X)
        to_core = lax.rem(core + rest, CORES)
        peer = (to_x * CHIPS_Z + to_z) * CORES + to_core

        @pl.when(peer != me)
        def _():
            pltpu.make_async_remote_copy(
                back_ref.at[peer], out_ref.at[me], reply_sem, out_sem,
                device_id={"wide": peer}, device_id_type=MESH,
            ).start()

        return carry

    lax.fori_loop(0, WIDE, reply, 0)
    sent = fields_ref.at[pl.ds(0, WIDE - 1)]
    pltpu.make_async_copy(sent, sent, send_sem).wait()
    replied = back_ref.at[pl.ds(0, WIDE - 1)]
    pltpu.make_async_copy(replied, replied, reply_sem).wait()
    filled = out_ref.at[pl.ds(0, WIDE - 1)]
    pltpu.make_async_copy(filled, filled, out_sem).wait()


CHUNK = (WIDE, SLOTS, 2, BLOCK)


def per_device(fields, counts, obs_index, obs_value, obs_weight):
    chunks = fields.reshape(2, WIDE, SLOTS, BLOCK).transpose(1, 2, 0, 3)
    vmem = pl.BlockSpec(memory_space=pltpu.VMEM)
    result = pl.pallas_call(
        kernel,
        out_shape=jax.ShapeDtypeStruct(CHUNK, BF16),
        in_specs=[vmem, pl.BlockSpec(memory_space=pltpu.SMEM), vmem, vmem, vmem],
        out_specs=vmem,
        scratch_shapes=[
            pltpu.VMEM(CHUNK, BF16),
            pltpu.VMEM(CHUNK, BF16),
            pltpu.VMEM((SLOTS, CELLS, NOBS), BF16),
            pltpu.VMEM((MEMBERS + 16, CELLS), BF16),
            pltpu.VMEM((1, CELLS), F32),
            pltpu.VMEM((LANES, MEMBERS, NOBS), BF16),
            pltpu.VMEM((LANES, MEMBERS, NOBS), BF16),
            pltpu.VMEM((LANES, MEMBERS, MEMBERS), BF16),
            pltpu.VMEM((LANES, MEMBERS, MEMBERS), BF16),
            pltpu.VMEM((LANES, MEMBERS, MEMBERS), BF16),
            pltpu.VMEM((LANES, 8, MEMBERS), F32),
            pltpu.VMEM((LANES, 8, 128), F32),
            pltpu.VMEM((SLOTS, MEMBERS, MEMBERS), BF16),
            pltpu.VMEM((SLOTS, NOBS), F32),
        ]
        + [pltpu.SemaphoreType.DMA] * 4,
        compiler_params=pltpu.CompilerParams(collective_id=0, has_side_effects=True, vmem_limit_bytes=48 * 2**20),
        name="tile_analysis",
    )(chunks, counts, obs_index, obs_value, obs_weight)
    return result.transpose(2, 0, 1, 3).reshape(2, WIDE * CELLS)


def solution(mesh):
    return jax.shard_map(
        per_device,
        mesh=mesh,
        in_specs=(
            P("wide", "narrow"),
            P(None, "wide"),
            P("narrow", "wide", None, None),
            P("narrow", "wide", None, None),
            P("narrow", "wide", None, None),
        ),
        out_specs=P("wide", "narrow"),
        check_vma=False,
    )
```

```python
import functools

import jax
import jax.numpy as jnp
from jax import lax
from jax.experimental import pallas as pl
from jax.experimental.pallas import tpu as pltpu
from jax.sharding import PartitionSpec as P

MEMBERS = 256
NOBS = 512
SLOTS = 8
CELLS = 1024
BLOCK = 128
NS_ITERS = 6
WIDE = 128
CHIPS_X, CHIPS_Z, CORES = 4, 16, 2
PHASES = 4
PARTS = 4
LANES = 4
MESH = pl.DeviceIdType.MESH
F32, BF16 = jnp.float32, jnp.bfloat16


def dot(a, b):
    return lax.dot_general(a, b, (((1,), (0,)), ((), ())), preferred_element_type=F32)


def dot_t(a, b):
    return lax.dot_general(a, b, (((1,), (1,)), ((), ())), preferred_element_type=F32)


def three_rows(row, fourth=0.0):
    high = row.astype(BF16).astype(F32)
    rest = row - high
    middle = rest.astype(BF16).astype(F32)
    low = rest - middle
    at = lax.broadcasted_iota(jnp.int32, (16, row.shape[1]), 0)
    rows = jnp.where(at == 0, high, jnp.where(at == 1, middle, jnp.where(at == 2, low, jnp.where(at == 3, fourth, 0.0))))
    return rows.astype(BF16)


def diagonal(value):
    rows = lax.broadcasted_iota(jnp.int32, (MEMBERS, MEMBERS), 0)
    columns = lax.broadcasted_iota(jnp.int32, (MEMBERS, MEMBERS), 1)
    return jnp.where(rows == columns, value, 0.0)


def sum_weights(index_ref, value_ref, weight_ref, mass_ref, pull_ref):
    def one(step, carry):
        slot, part = step // PARTS, lax.rem(step, PARTS)
        width = CELLS // PARTS
        weight = weight_ref[pl.ds(slot, 1), :]
        rows = three_rows(weight * value_ref[pl.ds(slot, 1), :], weight)
        cells = lax.broadcasted_iota(jnp.int32, (width, NOBS), 0) + part * width
        hit = jnp.where(cells == index_ref[pl.ds(slot, 1), :], 1.0, 0.0).astype(BF16)
        sums = dot_t(rows, hit)
        mass_ref[part, pl.ds(slot, 1), :] = sums[3:4]
        pull_ref[part, pl.ds(slot, 1), :] = sums[0:1] + sums[1:2] + sums[2:3]
        return carry

    lax.fori_loop(0, SLOTS * PARTS, one, 0)


def load_tile(in_ref, mass_ref, pull_ref, anomaly_ref, mean_ref, side_ref):
    for block in range(SLOTS):
        columns = slice(block * BLOCK, (block + 1) * BLOCK)
        part = in_ref[:, block].reshape(MEMBERS, BLOCK).astype(F32)
        mean = jnp.sum(part, axis=0, keepdims=True) / MEMBERS
        mean_ref[:, columns] = mean
        anomaly_ref[:, columns] = (part - mean).astype(BF16)
    side = jnp.zeros((SLOTS, MEMBERS), F32)
    for part in range(PARTS):
        columns = slice(part * (CELLS // PARTS), (part + 1) * (CELLS // PARTS))
        residual = pull_ref[part] - mass_ref[part] * mean_ref[:, columns]
        high = residual.astype(BF16).astype(F32)
        rest = residual - high
        middle = rest.astype(BF16).astype(F32)
        rows = jnp.concatenate([high, middle, rest - middle, jnp.zeros_like(high)], axis=0).astype(BF16)
        sums = dot_t(rows, anomaly_ref[:, columns])
        side = side + (sums[:SLOTS] + sums[SLOTS : 2 * SLOTS] + sums[2 * SLOTS : 3 * SLOTS])
    side_ref[...] = side


def solve(first, mass_ref, side_ref, anomaly_ref, iterate_ref, root_ref, factor_ref, inner_ref, scale_ref, patch_ref):
    half = diagonal(1.5)
    for lane in range(LANES):
        gram = diagonal(MEMBERS - 1.0)
        for part in range(PARTS):
            columns = slice(part * (CELLS // PARTS), (part + 1) * (CELLS // PARTS))
            anomaly = anomaly_ref[:, columns]
            mass = mass_ref[part, pl.ds(first + lane, 1), :]
            gram = gram + dot_t(anomaly, (anomaly.astype(F32) * mass).astype(BF16))
        scale = jnp.sqrt(jnp.sum(jnp.sum(gram * gram, axis=0, keepdims=True), axis=1, keepdims=True))
        scale_ref[lane] = jnp.broadcast_to(scale, (8, 128))
        iterate_ref[lane] = (gram * (1.0 / scale)).astype(BF16)
    for lane in range(LANES):
        root_ref[lane] = (half - 0.5 * iterate_ref[lane].astype(F32)).astype(BF16)
    for lane in range(LANES):
        iterate_ref[lane] = dot(root_ref[lane], iterate_ref[lane]).astype(BF16)

    def newton(iteration, carry):
        for lane in range(LANES):
            factor_ref[lane] = (half - 0.5 * dot(iterate_ref[lane], root_ref[lane])).astype(BF16)
        for lane in range(LANES):
            iterate_ref[lane] = dot(factor_ref[lane], iterate_ref[lane]).astype(BF16)
            root_ref[lane] = dot(root_ref[lane], factor_ref[lane]).astype(BF16)
        return carry

    lax.fori_loop(1, NS_ITERS - 1, newton, 0)
    for lane in range(LANES):
        factor_ref[lane] = (half - 0.5 * dot(iterate_ref[lane], root_ref[lane])).astype(BF16)
    for lane in range(LANES):
        root_ref[lane] = dot(root_ref[lane], factor_ref[lane]).astype(BF16)
    for lane in range(LANES):
        inner = dot(three_rows(side_ref[pl.ds(first + lane, 1), :]), root_ref[lane])
        inner_ref[lane] = jnp.broadcast_to(inner[0:1] + inner[1:2] + inner[2:3], (8, MEMBERS))
    for lane in range(LANES):
        scale = scale_ref[lane][:1, :1]
        shift = dot(three_rows(inner_ref[lane][:1]), root_ref[lane])
        shift = (shift[0:1] + shift[1:2] + shift[2:3]) / scale
        patch = jnp.sqrt((MEMBERS - 1.0) / scale) * root_ref[lane].astype(F32) + shift
        patch_ref[first + lane] = patch.astype(BF16)


def combine(start, count, patch_ref, anomaly_ref, mean_ref, back_ref):
    for lane in range(LANES):
        block = start + lane
        columns = pl.ds(pl.multiple_of(block * BLOCK, BLOCK), BLOCK)
        slot = (block * count) // SLOTS
        result = dot(patch_ref[slot], anomaly_ref[:, columns]) + mean_ref[:, columns]
        back_ref[:, block] = result.astype(BF16).reshape(MEMBERS // 2, 2, BLOCK)


def kernel(
    fields_hbm, counts_hbm, index_hbm, value_hbm, weight_hbm, out_ref,
    send_ref, in_ref, back_ref, counts_ref, index_ref, value_ref, weight_ref, wide_weight_ref, mass_ref, pull_ref,
    anomaly_ref, mean_ref, iterate_ref, root_ref, factor_ref, side_ref, inner_ref, scale_ref, patch_ref,
    load_sems, send_sem, in_sem, reply_sems, out_sem, keep_sem,
):
    me = lax.axis_index("wide")
    barrier = pltpu.get_barrier_semaphore()
    loads = [
        pltpu.make_async_copy(source, target, load_sems.at[number])
        for number, (source, target) in enumerate(
            ((index_hbm, index_ref), (value_hbm, value_ref), (weight_hbm, weight_ref), (counts_hbm, counts_ref), (fields_hbm, send_ref))
        )
    ]
    for load in loads:
        load.start()
    x, z, core = me // (CHIPS_Z * CORES), lax.rem(me // CORES, CHIPS_Z), lax.rem(me, CORES)
    sides = [
        lax.rem(x + dx, CHIPS_X) * (CHIPS_Z * CORES) + lax.rem(core + dc, CORES) for dx in range(CHIPS_X) for dc in range(CORES)
    ]

    def far_first(hop):
        side = (hop + 1) // 2
        return lax.rem(z + CHIPS_Z + CHIPS_Z // 2 + side * (1 - 2 * lax.rem(hop, 2)), CHIPS_Z)

    def greet(hop, carry):
        to_z = far_first(hop) * CORES
        for number, side in enumerate(sides):
            def one(peer=side + to_z):
                pl.semaphore_signal(barrier, inc=1, device_id={"wide": peer}, device_id_type=MESH)

            if number == 0:
                pl.when(to_z != z * CORES)(one)
            else:
                one()
        return carry

    lax.fori_loop(0, CHIPS_Z, greet, 0)
    for load in loads[:4]:
        load.wait()
    wide_weight_ref[...] = weight_ref[0, 0].astype(F32)
    sum_weights(index_ref.at[0, 0], value_ref.at[0, 0], wide_weight_ref, mass_ref, pull_ref)
    loads[4].wait()
    in_ref[me] = send_ref[me]
    pl.semaphore_wait(barrier, WIDE - 1)

    def send(step, carry):
        phase, hop = step // PHASES, lax.rem(step, PHASES)
        to_z = (PHASES * lax.rem(z // PHASES + hop, CHIPS_Z // PHASES) + phase) * CORES
        for number, side in enumerate(sides):
            def one(peer=side + to_z):
                pltpu.make_async_remote_copy(
                    send_ref.at[peer], in_ref.at[me], send_sem, in_sem,
                    device_id={"wide": peer}, device_id_type=MESH,
                ).start()

            if number == 0:
                pl.when(to_z != z * CORES)(one)
            else:
                one()
        return carry

    lax.fori_loop(0, CHIPS_Z, send, 0)
    others = in_ref.at[pl.ds(0, WIDE - 1)]
    pltpu.make_async_copy(others, others, in_sem).wait()
    load_tile(in_ref, mass_ref, pull_ref, anomaly_ref, mean_ref, side_ref)
    count = counts_ref[0, lax.axis_index("narrow")]

    def group(number, carry):
        first = number * LANES
        solve(first, mass_ref, side_ref, anomaly_ref, iterate_ref, root_ref, factor_ref, inner_ref, scale_ref, patch_ref)
        combine(first, count, patch_ref, anomaly_ref, mean_ref, back_ref)
        blocks = pl.ds(first, LANES)

        def reply(hop, carry):
            to_z = far_first(hop) * CORES
            for place, side in enumerate(sides):
                def one(peer=side + to_z):
                    pltpu.make_async_remote_copy(
                        back_ref.at[peer, blocks], out_ref.at[me, blocks], reply_sems.at[number], out_sem,
                        device_id={"wide": peer}, device_id_type=MESH,
                    ).start()

                if place == 0:
                    pl.when(to_z != z * CORES)(one)
                else:
                    one()
            return carry

        lax.fori_loop(0, CHIPS_Z, reply, 0)
        return carry

    lax.fori_loop(0, SLOTS // LANES, group, 0)
    keep = pltpu.make_async_copy(back_ref.at[me], out_ref.at[me], keep_sem)
    keep.start()
    sent = send_ref.at[pl.ds(0, WIDE - 1)]
    pltpu.make_async_copy(sent, sent, send_sem).wait()
    for number in range(SLOTS // LANES):
        replied = back_ref.at[pl.ds(0, WIDE - 1), pl.ds(0, LANES)]
        pltpu.make_async_copy(replied, replied, reply_sems.at[number]).wait()
    keep.wait()
    filled = out_ref.at[pl.ds(0, WIDE - 1)]
    pltpu.make_async_copy(filled, filled, out_sem).wait()


CHUNK = (WIDE, SLOTS, 2, BLOCK)


def per_device(fields, counts, obs_index, obs_value, obs_weight):
    chunks = fields.reshape(2, WIDE, SLOTS, BLOCK).transpose(1, 2, 0, 3)
    hbm = pl.BlockSpec(memory_space=pltpu.HBM)
    result = pl.pallas_call(
        kernel,
        out_shape=jax.ShapeDtypeStruct(CHUNK, BF16),
        in_specs=[hbm] * 5,
        out_specs=hbm,
        scratch_shapes=[
            pltpu.VMEM(CHUNK, BF16),
            pltpu.VMEM(CHUNK, BF16),
            pltpu.VMEM(CHUNK, BF16),
            pltpu.SMEM((1, 4), jnp.int32),
            pltpu.VMEM((1, 1, SLOTS, NOBS), jnp.int32),
            pltpu.VMEM((1, 1, SLOTS, NOBS), F32),
            pltpu.VMEM((1, 1, SLOTS, NOBS), BF16),
            pltpu.VMEM((SLOTS, NOBS), F32),
            pltpu.VMEM((PARTS, SLOTS, CELLS // PARTS), F32),
            pltpu.VMEM((PARTS, SLOTS, CELLS // PARTS), F32),
            pltpu.VMEM((MEMBERS, CELLS), BF16),
            pltpu.VMEM((1, CELLS), F32),
            pltpu.VMEM((LANES, MEMBERS, MEMBERS), BF16),
            pltpu.VMEM((LANES, MEMBERS, MEMBERS), BF16),
            pltpu.VMEM((LANES, MEMBERS, MEMBERS), BF16),
            pltpu.VMEM((SLOTS, MEMBERS), F32),
            pltpu.VMEM((LANES, 8, MEMBERS), F32),
            pltpu.VMEM((LANES, 8, 128), F32),
            pltpu.VMEM((SLOTS, MEMBERS, MEMBERS), BF16),
            pltpu.SemaphoreType.DMA((5,)),
            pltpu.SemaphoreType.DMA,
            pltpu.SemaphoreType.DMA,
            pltpu.SemaphoreType.DMA((2,)),
            pltpu.SemaphoreType.DMA,
            pltpu.SemaphoreType.DMA,
        ],
        compiler_params=pltpu.CompilerParams(collective_id=0, has_side_effects=True, vmem_limit_bytes=60 * 2**20),
        name="tile_analysis",
    )(chunks, counts.T, obs_index, obs_value, obs_weight)
    return result.transpose(2, 0, 1, 3).reshape(2, WIDE * CELLS)


def solution(mesh):
    return jax.shard_map(
        per_device,
        mesh=mesh,
        in_specs=(
            P("wide", "narrow"),
            P(None, "wide"),
            P("narrow", "wide", None, None),
            P("narrow", "wide", None, None),
            P("narrow", "wide", None, None),
        ),
        out_specs=P("wide", "narrow"),
        check_vma=False,
    )
```

```python
import functools

import jax
import jax.numpy as jnp
from jax import lax
from jax.experimental import pallas as pl
from jax.experimental.pallas import tpu as pltpu
from jax.sharding import PartitionSpec as P

MEMBERS = 256
NOBS = 512
SLOTS = 8
CELLS = 1024
BLOCK = 128
NS_ITERS = 6
WIDE = 128
CHIPS_X, CHIPS_Z, CORES = 4, 16, 2
PHASES = 4
PARTS = 4
LANES = 4
MESH = pl.DeviceIdType.MESH
F32, BF16 = jnp.float32, jnp.bfloat16


def dot(a, b):
    return lax.dot_general(a, b, (((1,), (0,)), ((), ())), preferred_element_type=F32)


def dot_t(a, b):
    return lax.dot_general(a, b, (((1,), (1,)), ((), ())), preferred_element_type=F32)


def three_rows(row, fourth=0.0):
    high = row.astype(BF16).astype(F32)
    rest = row - high
    middle = rest.astype(BF16).astype(F32)
    low = rest - middle
    at = lax.broadcasted_iota(jnp.int32, (16, row.shape[1]), 0)
    rows = jnp.where(at == 0, high, jnp.where(at == 1, middle, jnp.where(at == 2, low, jnp.where(at == 3, fourth, 0.0))))
    return rows.astype(BF16)


def diagonal(value):
    rows = lax.broadcasted_iota(jnp.int32, (MEMBERS, MEMBERS), 0)
    columns = lax.broadcasted_iota(jnp.int32, (MEMBERS, MEMBERS), 1)
    return jnp.where(rows == columns, value, 0.0)


def sum_weights(index_ref, value_ref, weight_ref, mass_ref, pull_ref):
    def one(step, carry):
        slot, part = step // PARTS, lax.rem(step, PARTS)
        width = CELLS // PARTS
        weight = weight_ref[pl.ds(slot, 1), :]
        rows = three_rows(weight * value_ref[pl.ds(slot, 1), :], weight)
        cells = lax.broadcasted_iota(jnp.int32, (width, NOBS), 0) + part * width
        hit = jnp.where(cells == index_ref[pl.ds(slot, 1), :], 1.0, 0.0).astype(BF16)
        sums = dot_t(rows, hit)
        mass_ref[part, pl.ds(slot, 1), :] = sums[3:4]
        pull_ref[part, pl.ds(slot, 1), :] = sums[0:1] + sums[1:2] + sums[2:3]
        return carry

    lax.fori_loop(0, SLOTS * PARTS, one, 0)


def load_tile(in_ref, mass_ref, pull_ref, anomaly_ref, mean_ref, side_ref):
    for block in range(SLOTS):
        columns = slice(block * BLOCK, (block + 1) * BLOCK)
        part = in_ref[:, block].reshape(MEMBERS, BLOCK).astype(F32)
        mean = jnp.sum(part, axis=0, keepdims=True) / MEMBERS
        mean_ref[:, columns] = mean
        anomaly_ref[:, columns] = (part - mean).astype(BF16)
    side = jnp.zeros((SLOTS, MEMBERS), F32)
    for part in range(PARTS):
        columns = slice(part * (CELLS // PARTS), (part + 1) * (CELLS // PARTS))
        residual = pull_ref[part] - mass_ref[part] * mean_ref[:, columns]
        high = residual.astype(BF16).astype(F32)
        rest = residual - high
        middle = rest.astype(BF16).astype(F32)
        rows = jnp.concatenate([high, middle, rest - middle, jnp.zeros_like(high)], axis=0).astype(BF16)
        sums = dot_t(rows, anomaly_ref[:, columns])
        side = side + (sums[:SLOTS] + sums[SLOTS : 2 * SLOTS] + sums[2 * SLOTS : 3 * SLOTS])
    side_ref[...] = side


def solve(first, mass_ref, side_ref, anomaly_ref, iterate_ref, root_ref, factor_ref, inner_ref, scale_ref, patch_ref):
    half = diagonal(1.5)
    for lane in range(LANES):
        gram = diagonal(MEMBERS - 1.0)
        for part in range(PARTS):
            columns = slice(part * (CELLS // PARTS), (part + 1) * (CELLS // PARTS))
            anomaly = anomaly_ref[:, columns]
            mass = mass_ref[part, pl.ds(first + lane, 1), :]
            gram = gram + dot_t(anomaly, (anomaly.astype(F32) * mass).astype(BF16))
        scale = jnp.sqrt(jnp.sum(jnp.sum(gram * gram, axis=0, keepdims=True), axis=1, keepdims=True))
        scale_ref[lane] = jnp.broadcast_to(scale, (8, 128))
        iterate_ref[lane] = (gram * (1.0 / scale)).astype(BF16)
    for lane in range(LANES):
        root_ref[lane] = (half - 0.5 * iterate_ref[lane].astype(F32)).astype(BF16)
    for lane in range(LANES):
        iterate_ref[lane] = dot(root_ref[lane], iterate_ref[lane]).astype(BF16)

    def newton(iteration, carry):
        for lane in range(LANES):
            factor_ref[lane] = (half - 0.5 * dot(iterate_ref[lane], root_ref[lane])).astype(BF16)
        for lane in range(LANES):
            iterate_ref[lane] = dot(factor_ref[lane], iterate_ref[lane]).astype(BF16)
            root_ref[lane] = dot(root_ref[lane], factor_ref[lane]).astype(BF16)
        return carry

    lax.fori_loop(1, NS_ITERS - 1, newton, 0)
    for lane in range(LANES):
        factor_ref[lane] = (half - 0.5 * dot(iterate_ref[lane], root_ref[lane])).astype(BF16)
    for lane in range(LANES):
        root_ref[lane] = dot(root_ref[lane], factor_ref[lane]).astype(BF16)
    for lane in range(LANES):
        inner = dot(three_rows(side_ref[pl.ds(first + lane, 1), :]), root_ref[lane])
        inner_ref[lane] = jnp.broadcast_to(inner[0:1] + inner[1:2] + inner[2:3], (8, MEMBERS))
    for lane in range(LANES):
        scale = scale_ref[lane][:1, :1]
        shift = dot(three_rows(inner_ref[lane][:1]), root_ref[lane])
        shift = (shift[0:1] + shift[1:2] + shift[2:3]) / scale
        patch = jnp.sqrt((MEMBERS - 1.0) / scale) * root_ref[lane].astype(F32) + shift
        patch_ref[first + lane] = patch.astype(BF16)


def combine(start, count, patch_ref, anomaly_ref, mean_ref, back_ref):
    for lane in range(LANES):
        block = start + lane
        columns = pl.ds(pl.multiple_of(block * BLOCK, BLOCK), BLOCK)
        slot = (block * count) // SLOTS
        result = dot(patch_ref[slot], anomaly_ref[:, columns]) + mean_ref[:, columns]
        back_ref[:, block] = result.astype(BF16).reshape(MEMBERS // 2, 2, BLOCK)


def kernel(
    fields_hbm, counts_hbm, index_hbm, value_hbm, weight_hbm, out_ref,
    send_ref, in_ref, back_ref, counts_ref, index_ref, value_ref, weight_ref, wide_weight_ref, mass_ref, pull_ref,
    anomaly_ref, mean_ref, iterate_ref, root_ref, factor_ref, side_ref, inner_ref, scale_ref, patch_ref,
    load_sems, send_sem, in_sem, reply_sems, out_sem, keep_sem,
):
    me = lax.axis_index("wide")
    barrier = pltpu.get_barrier_semaphore()
    loads = [
        pltpu.make_async_copy(source, target, load_sems.at[number])
        for number, (source, target) in enumerate(
            ((index_hbm, index_ref), (value_hbm, value_ref), (weight_hbm, weight_ref), (counts_hbm, counts_ref), (fields_hbm, send_ref))
        )
    ]
    for load in loads:
        load.start()
    x, z, core = me // (CHIPS_Z * CORES), lax.rem(me // CORES, CHIPS_Z), lax.rem(me, CORES)
    sides = [
        lax.rem(x + dx, CHIPS_X) * (CHIPS_Z * CORES) + lax.rem(core + dc, CORES) for dx in range(CHIPS_X) for dc in range(CORES)
    ]

    def far_first(hop):
        side = (hop + 1) // 2
        return lax.rem(z + CHIPS_Z + CHIPS_Z // 2 + side * (1 - 2 * lax.rem(hop, 2)), CHIPS_Z)

    def greet(hop, carry):
        to_z = far_first(hop) * CORES
        for number, side in enumerate(sides):
            def one(peer=side + to_z):
                pl.semaphore_signal(barrier, inc=1, device_id={"wide": peer}, device_id_type=MESH)

            if number == 0:
                pl.when(to_z != z * CORES)(one)
            else:
                one()
        return carry

    lax.fori_loop(0, CHIPS_Z, greet, 0)
    for load in loads[:4]:
        load.wait()
    wide_weight_ref[...] = weight_ref[0, 0].astype(F32)
    sum_weights(index_ref.at[0, 0], value_ref.at[0, 0], wide_weight_ref, mass_ref, pull_ref)
    loads[4].wait()
    in_ref[me] = send_ref[me]
    pl.semaphore_wait(barrier, WIDE - 1)

    columns = [lax.rem(x + dx, CHIPS_X) * (CHIPS_Z * CORES) for dx in range(CHIPS_X)]

    def send(step, carry):
        phase, rest = step // (CORES * PHASES), lax.rem(step, CORES * PHASES)
        to_core, hop = rest // PHASES, lax.rem(rest, PHASES)
        below = (PHASES * lax.rem(z // PHASES + hop, CHIPS_Z // PHASES) + phase) * CORES + to_core
        for number, column in enumerate(columns):
            def one(peer=column + below):
                pltpu.make_async_remote_copy(
                    send_ref.at[peer], in_ref.at[me], send_sem, in_sem,
                    device_id={"wide": peer}, device_id_type=MESH,
                ).start()

            if number == 0:
                pl.when(below != z * CORES + core)(one)
            else:
                one()
        return carry

    lax.fori_loop(0, CHIPS_Z * CORES, send, 0)
    others = in_ref.at[pl.ds(0, WIDE - 1)]
    pltpu.make_async_copy(others, others, in_sem).wait()
    load_tile(in_ref, mass_ref, pull_ref, anomaly_ref, mean_ref, side_ref)
    count = counts_ref[0, lax.axis_index("narrow")]

    def group(number, carry):
        first = number * LANES
        solve(first, mass_ref, side_ref, anomaly_ref, iterate_ref, root_ref, factor_ref, inner_ref, scale_ref, patch_ref)
        combine(first, count, patch_ref, anomaly_ref, mean_ref, back_ref)
        blocks = pl.ds(first, LANES)

        def reply(hop, carry):
            to_z = far_first(hop) * CORES
            for place, side in enumerate(sides):
                def one(peer=side + to_z):
                    pltpu.make_async_remote_copy(
                        back_ref.at[peer, blocks], out_ref.at[me, blocks], reply_sems.at[number], out_sem,
                        device_id={"wide": peer}, device_id_type=MESH,
                    ).start()

                if place == 0:
                    pl.when(to_z != z * CORES)(one)
                else:
                    one()
            return carry

        lax.fori_loop(0, CHIPS_Z, reply, 0)
        return carry

    lax.fori_loop(0, SLOTS // LANES, group, 0)
    keep = pltpu.make_async_copy(back_ref.at[me], out_ref.at[me], keep_sem)
    keep.start()
    sent = send_ref.at[pl.ds(0, WIDE - 1)]
    pltpu.make_async_copy(sent, sent, send_sem).wait()
    for number in range(SLOTS // LANES):
        replied = back_ref.at[pl.ds(0, WIDE - 1), pl.ds(0, LANES)]
        pltpu.make_async_copy(replied, replied, reply_sems.at[number]).wait()
    keep.wait()
    filled = out_ref.at[pl.ds(0, WIDE - 1)]
    pltpu.make_async_copy(filled, filled, out_sem).wait()


CHUNK = (WIDE, SLOTS, 2, BLOCK)


def per_device(fields, counts, obs_index, obs_value, obs_weight):
    chunks = fields.reshape(2, WIDE, SLOTS, BLOCK).transpose(1, 2, 0, 3)
    hbm = pl.BlockSpec(memory_space=pltpu.HBM)
    result = pl.pallas_call(
        kernel,
        out_shape=jax.ShapeDtypeStruct(CHUNK, BF16),
        in_specs=[hbm] * 5,
        out_specs=hbm,
        scratch_shapes=[
            pltpu.VMEM(CHUNK, BF16),
            pltpu.VMEM(CHUNK, BF16),
            pltpu.VMEM(CHUNK, BF16),
            pltpu.SMEM((1, 4), jnp.int32),
            pltpu.VMEM((1, 1, SLOTS, NOBS), jnp.int32),
            pltpu.VMEM((1, 1, SLOTS, NOBS), F32),
            pltpu.VMEM((1, 1, SLOTS, NOBS), BF16),
            pltpu.VMEM((SLOTS, NOBS), F32),
            pltpu.VMEM((PARTS, SLOTS, CELLS // PARTS), F32),
            pltpu.VMEM((PARTS, SLOTS, CELLS // PARTS), F32),
            pltpu.VMEM((MEMBERS, CELLS), BF16),
            pltpu.VMEM((1, CELLS), F32),
            pltpu.VMEM((LANES, MEMBERS, MEMBERS), BF16),
            pltpu.VMEM((LANES, MEMBERS, MEMBERS), BF16),
            pltpu.VMEM((LANES, MEMBERS, MEMBERS), BF16),
            pltpu.VMEM((SLOTS, MEMBERS), F32),
            pltpu.VMEM((LANES, 8, MEMBERS), F32),
            pltpu.VMEM((LANES, 8, 128), F32),
            pltpu.VMEM((SLOTS, MEMBERS, MEMBERS), BF16),
            pltpu.SemaphoreType.DMA((5,)),
            pltpu.SemaphoreType.DMA,
            pltpu.SemaphoreType.DMA,
            pltpu.SemaphoreType.DMA((2,)),
            pltpu.SemaphoreType.DMA,
            pltpu.SemaphoreType.DMA,
        ],
        compiler_params=pltpu.CompilerParams(collective_id=0, has_side_effects=True, vmem_limit_bytes=60 * 2**20),
        name="tile_analysis",
    )(chunks, counts.T, obs_index, obs_value, obs_weight)
    return result.transpose(2, 0, 1, 3).reshape(2, WIDE * CELLS)


def solution(mesh):
    return jax.shard_map(
        per_device,
        mesh=mesh,
        in_specs=(
            P("wide", "narrow"),
            P(None, "wide"),
            P("narrow", "wide", None, None),
            P("narrow", "wide", None, None),
            P("narrow", "wide", None, None),
        ),
        out_specs=P("wide", "narrow"),
        check_vma=False,
    )
```

```python
import functools

import jax
import jax.numpy as jnp
from jax import lax
from jax.experimental import pallas as pl
from jax.experimental.pallas import tpu as pltpu
from jax.sharding import PartitionSpec as P

MEMBERS = 256
NOBS = 512
SLOTS = 8
CELLS = 1024
BLOCK = 128
NS_ITERS = 6
WIDE = 128
CHIPS_X, CHIPS_Z, CORES = 4, 16, 2
PHASES = 4
PARTS = 4
LANES = 4
MESH = pl.DeviceIdType.MESH
F32, BF16 = jnp.float32, jnp.bfloat16


def dot(a, b):
    return lax.dot_general(a, b, (((1,), (0,)), ((), ())), preferred_element_type=F32)


def dot_t(a, b):
    return lax.dot_general(a, b, (((1,), (1,)), ((), ())), preferred_element_type=F32)


def three_rows(row, fourth=0.0):
    high = row.astype(BF16).astype(F32)
    rest = row - high
    middle = rest.astype(BF16).astype(F32)
    low = rest - middle
    at = lax.broadcasted_iota(jnp.int32, (16, row.shape[1]), 0)
    rows = jnp.where(at == 0, high, jnp.where(at == 1, middle, jnp.where(at == 2, low, jnp.where(at == 3, fourth, 0.0))))
    return rows.astype(BF16)


def diagonal(value):
    rows = lax.broadcasted_iota(jnp.int32, (MEMBERS, MEMBERS), 0)
    columns = lax.broadcasted_iota(jnp.int32, (MEMBERS, MEMBERS), 1)
    return jnp.where(rows == columns, value, 0.0)


def sum_weights(index_ref, value_ref, weight_ref, mass_ref, pull_ref):
    def one(step, carry):
        slot, part = step // PARTS, lax.rem(step, PARTS)
        width = CELLS // PARTS
        weight = weight_ref[pl.ds(slot, 1), :]
        rows = three_rows(weight * value_ref[pl.ds(slot, 1), :], weight)
        cells = lax.broadcasted_iota(jnp.int32, (width, NOBS), 0) + part * width
        hit = jnp.where(cells == index_ref[pl.ds(slot, 1), :], 1.0, 0.0).astype(BF16)
        sums = dot_t(rows, hit)
        mass_ref[part, pl.ds(slot, 1), :] = sums[3:4]
        pull_ref[part, pl.ds(slot, 1), :] = sums[0:1] + sums[1:2] + sums[2:3]
        return carry

    lax.fori_loop(0, SLOTS * PARTS, one, 0)


def load_tile(in_ref, mass_ref, pull_ref, anomaly_ref, mean_ref, side_ref):
    for block in range(SLOTS):
        columns = slice(block * BLOCK, (block + 1) * BLOCK)
        part = in_ref[:, block].reshape(MEMBERS, BLOCK).astype(F32)
        mean = jnp.sum(part, axis=0, keepdims=True) / MEMBERS
        mean_ref[:, columns] = mean
        anomaly_ref[:, columns] = (part - mean).astype(BF16)
    side = jnp.zeros((SLOTS, MEMBERS), F32)
    for part in range(PARTS):
        columns = slice(part * (CELLS // PARTS), (part + 1) * (CELLS // PARTS))
        residual = pull_ref[part] - mass_ref[part] * mean_ref[:, columns]
        high = residual.astype(BF16).astype(F32)
        rest = residual - high
        middle = rest.astype(BF16).astype(F32)
        rows = jnp.concatenate([high, middle, rest - middle, jnp.zeros_like(high)], axis=0).astype(BF16)
        sums = dot_t(rows, anomaly_ref[:, columns])
        side = side + (sums[:SLOTS] + sums[SLOTS : 2 * SLOTS] + sums[2 * SLOTS : 3 * SLOTS])
    side_ref[...] = side


def solve(first, mass_ref, side_ref, anomaly_ref, iterate_ref, root_ref, factor_ref, inner_ref, scale_ref, patch_ref):
    half = diagonal(1.5)
    for lane in range(LANES):
        gram = diagonal(MEMBERS - 1.0)
        for part in range(PARTS):
            columns = slice(part * (CELLS // PARTS), (part + 1) * (CELLS // PARTS))
            anomaly = anomaly_ref[:, columns]
            mass = mass_ref[part, pl.ds(first + lane, 1), :]
            gram = gram + dot_t(anomaly, (anomaly.astype(F32) * mass).astype(BF16))
        scale = jnp.sqrt(jnp.sum(jnp.sum(gram * gram, axis=0, keepdims=True), axis=1, keepdims=True))
        scale_ref[lane] = jnp.broadcast_to(scale, (8, 128))
        iterate_ref[lane] = (gram * (1.0 / scale)).astype(BF16)
    for lane in range(LANES):
        root_ref[lane] = (half - 0.5 * iterate_ref[lane].astype(F32)).astype(BF16)
    for lane in range(LANES):
        iterate_ref[lane] = dot(root_ref[lane], iterate_ref[lane]).astype(BF16)

    def newton(iteration, carry):
        for lane in range(LANES):
            factor_ref[lane] = (half - 0.5 * dot(iterate_ref[lane], root_ref[lane])).astype(BF16)
        for lane in range(LANES):
            iterate_ref[lane] = dot(factor_ref[lane], iterate_ref[lane]).astype(BF16)
            root_ref[lane] = dot(root_ref[lane], factor_ref[lane]).astype(BF16)
        return carry

    lax.fori_loop(1, NS_ITERS - 1, newton, 0)
    for lane in range(LANES):
        factor_ref[lane] = (half - 0.5 * dot(iterate_ref[lane], root_ref[lane])).astype(BF16)
    for lane in range(LANES):
        root_ref[lane] = dot(root_ref[lane], factor_ref[lane]).astype(BF16)
    for lane in range(LANES):
        inner = dot(three_rows(side_ref[pl.ds(first + lane, 1), :]), root_ref[lane])
        inner_ref[lane] = jnp.broadcast_to(inner[0:1] + inner[1:2] + inner[2:3], (8, MEMBERS))
    for lane in range(LANES):
        scale = scale_ref[lane][:1, :1]
        shift = dot(three_rows(inner_ref[lane][:1]), root_ref[lane])
        shift = (shift[0:1] + shift[1:2] + shift[2:3]) / scale
        patch = jnp.sqrt((MEMBERS - 1.0) / scale) * root_ref[lane].astype(F32) + shift
        patch_ref[first + lane] = patch.astype(BF16)


def combine(start, count, patch_ref, anomaly_ref, mean_ref, back_ref):
    for lane in range(LANES):
        block = start + lane
        columns = pl.ds(pl.multiple_of(block * BLOCK, BLOCK), BLOCK)
        slot = (block * count) // SLOTS
        result = dot(patch_ref[slot], anomaly_ref[:, columns]) + mean_ref[:, columns]
        back_ref[:, block] = result.astype(BF16).reshape(MEMBERS // 2, 2, BLOCK)


def kernel(
    fields_hbm, counts_hbm, index_hbm, value_hbm, weight_hbm, out_ref,
    send_ref, in_ref, back_ref, counts_ref, index_ref, value_ref, weight_ref, wide_weight_ref, mass_ref, pull_ref,
    anomaly_ref, mean_ref, iterate_ref, root_ref, factor_ref, side_ref, inner_ref, scale_ref, patch_ref,
    load_sems, send_sem, in_sem, reply_sems, out_sem, keep_sem,
):
    me = lax.axis_index("wide")
    barrier = pltpu.get_barrier_semaphore()
    loads = [
        pltpu.make_async_copy(source, target, load_sems.at[number])
        for number, (source, target) in enumerate(
            ((index_hbm, index_ref), (value_hbm, value_ref), (weight_hbm, weight_ref), (counts_hbm, counts_ref), (fields_hbm, send_ref))
        )
    ]
    for load in loads:
        load.start()
    x, z, core = me // (CHIPS_Z * CORES), lax.rem(me // CORES, CHIPS_Z), lax.rem(me, CORES)
    sides = [
        lax.rem(x + dx, CHIPS_X) * (CHIPS_Z * CORES) + lax.rem(core + dc, CORES) for dx in range(CHIPS_X) for dc in range(CORES)
    ]

    def far_first(hop):
        side = (hop + 1) // 2
        return lax.rem(z + CHIPS_Z + CHIPS_Z // 2 + side * (1 - 2 * lax.rem(hop, 2)), CHIPS_Z)

    def greet(hop, carry):
        to_z = far_first(hop) * CORES
        for number, side in enumerate(sides):
            def one(peer=side + to_z):
                pl.semaphore_signal(barrier, inc=1, device_id={"wide": peer}, device_id_type=MESH)

            if number == 0:
                pl.when(to_z != z * CORES)(one)
            else:
                one()
        return carry

    lax.fori_loop(0, CHIPS_Z, greet, 0)
    loads[4].wait()
    in_ref[me] = send_ref[me]
    pl.semaphore_wait(barrier, WIDE - 1)

    columns = [lax.rem(x + dx, CHIPS_X) * (CHIPS_Z * CORES) for dx in range(CHIPS_X)]

    def send(step, carry):
        phase, rest = step // (CORES * PHASES), lax.rem(step, CORES * PHASES)
        to_core, hop = rest // PHASES, lax.rem(rest, PHASES)
        below = (PHASES * lax.rem(z // PHASES + hop, CHIPS_Z // PHASES) + phase) * CORES + to_core
        for number, column in enumerate(columns):
            def one(peer=column + below):
                pltpu.make_async_remote_copy(
                    send_ref.at[peer], in_ref.at[me], send_sem, in_sem,
                    device_id={"wide": peer}, device_id_type=MESH,
                ).start()

            if number == 0:
                pl.when(below != z * CORES + core)(one)
            else:
                one()
        return carry

    lax.fori_loop(0, CHIPS_Z * CORES, send, 0)
    for load in loads[:4]:
        load.wait()
    wide_weight_ref[...] = weight_ref[0, 0].astype(F32)
    sum_weights(index_ref.at[0, 0], value_ref.at[0, 0], wide_weight_ref, mass_ref, pull_ref)
    others = in_ref.at[pl.ds(0, WIDE - 1)]
    pltpu.make_async_copy(others, others, in_sem).wait()
    load_tile(in_ref, mass_ref, pull_ref, anomaly_ref, mean_ref, side_ref)
    count = counts_ref[0, lax.axis_index("narrow")]

    def group(number, carry):
        first = number * LANES
        solve(first, mass_ref, side_ref, anomaly_ref, iterate_ref, root_ref, factor_ref, inner_ref, scale_ref, patch_ref)
        combine(first, count, patch_ref, anomaly_ref, mean_ref, back_ref)
        blocks = pl.ds(first, LANES)

        def reply(hop, carry):
            to_z = far_first(hop) * CORES
            for place, side in enumerate(sides):
                def one(peer=side + to_z):
                    pltpu.make_async_remote_copy(
                        back_ref.at[peer, blocks], out_ref.at[me, blocks], reply_sems.at[number], out_sem,
                        device_id={"wide": peer}, device_id_type=MESH,
                    ).start()

                if place == 0:
                    pl.when(to_z != z * CORES)(one)
                else:
                    one()
            return carry

        lax.fori_loop(0, CHIPS_Z, reply, 0)
        return carry

    lax.fori_loop(0, SLOTS // LANES, group, 0)
    keep = pltpu.make_async_copy(back_ref.at[me], out_ref.at[me], keep_sem)
    keep.start()
    sent = send_ref.at[pl.ds(0, WIDE - 1)]
    pltpu.make_async_copy(sent, sent, send_sem).wait()
    for number in range(SLOTS // LANES):
        replied = back_ref.at[pl.ds(0, WIDE - 1), pl.ds(0, LANES)]
        pltpu.make_async_copy(replied, replied, reply_sems.at[number]).wait()
    keep.wait()
    filled = out_ref.at[pl.ds(0, WIDE - 1)]
    pltpu.make_async_copy(filled, filled, out_sem).wait()


CHUNK = (WIDE, SLOTS, 2, BLOCK)


def per_device(fields, counts, obs_index, obs_value, obs_weight):
    chunks = fields.reshape(2, WIDE, SLOTS, BLOCK).transpose(1, 2, 0, 3)
    hbm = pl.BlockSpec(memory_space=pltpu.HBM)
    result = pl.pallas_call(
        kernel,
        out_shape=jax.ShapeDtypeStruct(CHUNK, BF16),
        in_specs=[hbm] * 5,
        out_specs=hbm,
        scratch_shapes=[
            pltpu.VMEM(CHUNK, BF16),
            pltpu.VMEM(CHUNK, BF16),
            pltpu.VMEM(CHUNK, BF16),
            pltpu.SMEM((1, 4), jnp.int32),
            pltpu.VMEM((1, 1, SLOTS, NOBS), jnp.int32),
            pltpu.VMEM((1, 1, SLOTS, NOBS), F32),
            pltpu.VMEM((1, 1, SLOTS, NOBS), BF16),
            pltpu.VMEM((SLOTS, NOBS), F32),
            pltpu.VMEM((PARTS, SLOTS, CELLS // PARTS), F32),
            pltpu.VMEM((PARTS, SLOTS, CELLS // PARTS), F32),
            pltpu.VMEM((MEMBERS, CELLS), BF16),
            pltpu.VMEM((1, CELLS), F32),
            pltpu.VMEM((LANES, MEMBERS, MEMBERS), BF16),
            pltpu.VMEM((LANES, MEMBERS, MEMBERS), BF16),
            pltpu.VMEM((LANES, MEMBERS, MEMBERS), BF16),
            pltpu.VMEM((SLOTS, MEMBERS), F32),
            pltpu.VMEM((LANES, 8, MEMBERS), F32),
            pltpu.VMEM((LANES, 8, 128), F32),
            pltpu.VMEM((SLOTS, MEMBERS, MEMBERS), BF16),
            pltpu.SemaphoreType.DMA((5,)),
            pltpu.SemaphoreType.DMA,
            pltpu.SemaphoreType.DMA,
            pltpu.SemaphoreType.DMA((2,)),
            pltpu.SemaphoreType.DMA,
            pltpu.SemaphoreType.DMA,
        ],
        compiler_params=pltpu.CompilerParams(collective_id=0, has_side_effects=True, vmem_limit_bytes=60 * 2**20),
        name="tile_analysis",
    )(chunks, counts.T, obs_index, obs_value, obs_weight)
    return result.transpose(2, 0, 1, 3).reshape(2, WIDE * CELLS)


def solution(mesh):
    return jax.shard_map(
        per_device,
        mesh=mesh,
        in_specs=(
            P("wide", "narrow"),
            P(None, "wide"),
            P("narrow", "wide", None, None),
            P("narrow", "wide", None, None),
            P("narrow", "wide", None, None),
        ),
        out_specs=P("wide", "narrow"),
        check_vma=False,
    )
```
